128 devices in a mesh: row: 16 (over x, z), col: 8 (over y, core).
Axes of the slice: x: 4, y: 4, z: 4, core: 2. Of those that a mesh axis runs over, the one named last changes fastest.
Arguments:
- krylov_basis: float32 [4, 2, 3, 128, 128, 256], P(None, None, None, 'col', 'row'), may hold values from -50 to 50
- susceptibility: float32 [128, 128, 256], P('col', 'row'), may hold values from 0.1 to 1
- green_spectra: bfloat16 [6, 256, 256, 512], P(None, None, 'col', 'row'), may hold values from -3 to 3, as said below
Outputs:
- projections: float32 [4, 2, 2], replicated
- next_block: float32 [2, 3, 128, 128, 256], P(None, None, 'col', 'row')
- block_factor: float32 [2, 2], replicated
The draws below stay inside these ranges and needn't reach their ends.
Inputs may be any that keep to these rules, and one draw needn't show every extreme that they name: `green_spectra`: each of the six arrays is even on the padded grid: its value at (a, b, c) equals its value at ((-a) mod 256, (-b) mod 256, (-c) mod 512).
All inputs are finite; a program needn't handle non-finite values.
Results may differ from the reference program's by a relative error of at most 0.0003.
Values sent between devices are 32-bit elements; how exact they have to be, the bound alone decides.
No kernel may reach another device: no remote copies, remote signals or barrier semaphores. Data moves between devices by JAX's collectives and lax.ppermute only.
A program may use at most 128 MiB of HBM per device.

```python
import math
import jax
import jax.numpy as jnp
from jax import lax

GX = 256
GY = 128
GZ = 128
NB = 4


def draw_krylov_basis(key, part):
    shared = jnp.clip(jax.random.normal(jax.random.fold_in(key, 12), (2, 3, GZ, GY, GX), jnp.float32), -6.0, 6.0)
    depths = (jnp.arange(GZ, dtype=jnp.float32) + 0.5) / GZ
    across = (jnp.arange(GY, dtype=jnp.float32) + 0.5) / GY
    envelope = (0.3 + depths[:, None] + across[None, :])[:, :, None]
    own = jnp.clip(jax.random.normal(jax.random.fold_in(key, 11), (NB, 2, 3, GZ, GY, GX), jnp.float32), -6.0, 6.0)
    return (own + shared) * (envelope * math.sqrt(0.5))


def draw_green_spectra(key, part):

    def one_entry(entry_key):
        raw = jnp.clip(jax.random.normal(entry_key, (2 * GZ, 2 * GY, 2 * GX), jnp.float32), -6.0, 6.0)
        mirrored = jnp.roll(jnp.flip(raw), (1, 1, 1), axis=(0, 1, 2))
        return (0.25 * (raw + mirrored)).astype(jnp.bfloat16)
    entry_keys = jax.random.split(jax.random.fold_in(key, 21), 6)
    return lax.map(one_entry, entry_keys)


def block_scale(stream_key, extent, cuts, low, high):
    def one(dim, blocks):
        draws = jax.random.uniform(jax.random.fold_in(jax.random.fold_in(stream_key, 6), dim), (blocks,), jnp.float32, low / len(cuts), high / len(cuts))
        return jnp.repeat(jnp.exp(draws), extent[dim] // blocks).reshape((-1,) + (1,) * (len(extent) - dim - 1))

    factor_of = one(*cuts[0])
    for cut in cuts[1:]:
        factor_of = factor_of * one(*cut)
    return factor_of


def setup_inputs(seed: int = 0) -> dict:
    key_list = jax.random.split(jax.random.key(seed), 4)
    return {
        "krylov_basis": draw_krylov_basis(jax.random.fold_in(key_list[3], 71), 0),
        "susceptibility": jnp.clip(jnp.exp(math.log(1.0) - 2.3025851 * jax.random.uniform(key_list[1], (GZ, GY, GX), jnp.float32) ** block_scale(key_list[1], (GZ, GY, GX), ((0, 8), (1, 16)), -0.2, 0.2)), 0.1, 1.0),
        "green_spectra": draw_green_spectra(jax.random.fold_in(key_list[3], 71), 0),
    }


highest = lax.Precision.HIGHEST
tensor_pairs = ((0, 3, 4), (3, 1, 5), (4, 5, 2))

def convolve(field, green_spectra):
    padded_shape = (2 * GZ, 2 * GY, 2 * GX)
    half_kernel = green_spectra[:, :, :, :GX + 1].astype(jnp.float32)
    spectra = jnp.fft.rfftn(field, s=padded_shape, axes=(1, 2, 3))
    results = []
    for member in range(3):
        chosen = tensor_pairs[member]
        mixed = half_kernel[chosen[0]] * spectra[0] + half_kernel[chosen[1]] * spectra[1] + half_kernel[chosen[2]] * spectra[2]
        full_field = jnp.fft.irfftn(mixed, s=padded_shape, axes=(0, 1, 2))
        results.append(full_field[:GZ, :GY, :GX])
    return jnp.stack(results)

def reference(krylov_basis, susceptibility, green_spectra):
    latest = krylov_basis[NB - 1]
    response = jnp.stack([convolve(latest[0], green_spectra), convolve(latest[1], green_spectra)])
    image = latest - susceptibility[None, None] * response
    entry_count = 3.0 * GX * GY * GZ
    flat_basis = krylov_basis.reshape(2 * NB, -1)
    flat_image = image.reshape(2, -1)
    coefficients = jnp.dot(flat_basis, flat_image.T, precision=highest) / entry_count
    projected = flat_image - jnp.dot(coefficients.T, flat_basis, precision=highest)
    gram = jnp.dot(projected, projected.T, precision=highest) / entry_count
    lead_norm = jnp.sqrt(gram[0, 0] + 1e-06)
    cross_term = gram[0, 1] / lead_norm
    tail_norm = jnp.sqrt(gram[1, 1] - cross_term * cross_term + 1e-06)
    first_column = projected[0] / lead_norm
    second_column = (projected[1] - cross_term * first_column) / tail_norm
    next_block = jnp.stack([first_column, second_column]).reshape(image.shape)
    block_factor = jnp.stack([jnp.stack([lead_norm, cross_term]), jnp.stack([jnp.zeros_like(lead_norm), tail_norm])])
    return (coefficients.reshape(NB, 2, 2), next_block, block_factor)
```

```python
import math

import jax
import jax.numpy as jnp
import ml_dtypes
import numpy as np
from jax import lax
from jax.experimental import pallas as pl
from jax.experimental.pallas import tpu as pltpu
from jax.sharding import Mesh
from jax.sharding import PartitionSpec as P

GX = 256
GY = 128
GZ = 128
NB = 4
ROW = ("row_0", "row_1")
COL = ("col_0", "col_1")
ROW_COL = ROW + COL
NROW = 16
NCOL = 8
LZ = GZ // NCOL
LY = GY // NROW
PX = 2 * GX // NROW
HX = PX // 2
PY = 2 * GY // NCOL
F32 = jnp.float32
BF16 = jnp.bfloat16
tensor_pairs = ((0, 3, 4), (3, 1, 5), (4, 5, 2))
ENTRY = 3.0 * GX * GY * GZ
SCALING = 1.0 / (8 * GX * GY * GZ)
PAIRS = [(i, k) for i in range(2 * NB) for k in range(i, 2 * NB)]
VMEM = 63 * 1024 * 1024


def split_np(table):
    table = table.astype(np.float32)
    high = table.astype(ml_dtypes.bfloat16)
    low = (table - high.astype(np.float32)).astype(ml_dtypes.bfloat16)
    return [high, low]


def tables():
    kx = np.arange(2 * GX).reshape(NROW, 2, PX // 2).transpose(1, 0, 2).reshape(-1)
    angle = (np.outer(np.arange(GX), kx) % (2 * GX)) * (2.0 * math.pi / (2 * GX))
    x_tables = split_np(np.cos(angle)) + split_np(np.sin(angle))
    angle = (np.outer(np.arange(2 * GY), np.arange(GY)) % (2 * GY)) * (2.0 * math.pi / (2 * GY))
    side = np.concatenate([np.cos(angle), np.sin(angle)], axis=0)
    return x_tables, split_np(side), split_np(side.T.copy())


def split(x):
    high = x.astype(BF16)
    low = (x - high.astype(F32)).astype(BF16)
    return high, low


def dot(a, b, ca, cb):
    return lax.dot_general(a, b, (((ca,), (cb,)), ((), ())), preferred_element_type=F32)


def ahead(ref):
    c, s = ref[:256], ref[256:]
    return jnp.concatenate([jnp.concatenate([c, s], axis=1), jnp.concatenate([-s, c], axis=1)], axis=0)


def behind(ref):
    c, s = ref[:, :256], ref[:, 256:]
    return jnp.concatenate([jnp.concatenate([c, -s], axis=1), jnp.concatenate([s, c], axis=1)], axis=0)


def left(th, tl, x, cb):
    h, l = split(x)
    n = th.shape[0]
    wide = dot(jnp.concatenate([th, tl], axis=0), h, 1, cb)
    return wide[:n] + (wide[n:] + dot(th, l, 1, cb))


def right(x, th, tl, cb):
    h, l = split(x)
    n = x.shape[0]
    wide = dot(jnp.concatenate([h, l], axis=0), th, 1, cb)
    return wide[:n] + (wide[n:] + dot(h, tl, 1, cb))


def swap_blocks(v, width):
    v = list(v)
    block = lax.broadcasted_iota(jnp.int32, v[0].shape, 1) // width
    step = len(v) // 2
    while step:
        keep = (block & step) == 0
        for i in range(len(v)):
            if i & step == 0:
                p, q = v[i], v[i + step]
                v[i] = jnp.where(keep, p, pltpu.roll(q, step * width, 1))
                v[i + step] = jnp.where(keep, pltpu.roll(p, 128 - step * width, 1), q)
        step //= 2
    return v


def x_forward(*refs):
    u_ref, ch_ref, cl_ref, sh_ref, sl_ref, o_ref = refs[-6:]
    n = LZ * LY
    u = jnp.concatenate([u_ref[0, 0, 0].reshape(n, GX), u_ref[0, 1, 0].reshape(n, GX)], axis=0)
    c = right(u, ch_ref[...], cl_ref[...], 0)
    s = right(u, sh_ref[...], sl_ref[...], 0)
    acc = jnp.concatenate([c[:n] + s[n:], c[n:] - s[:n]], axis=0)
    acc = acc.reshape(2, 2, 8, LY, GX)
    for t in range(2):
        part = acc[..., t * 128 : (t + 1) * 128]
        v = [part[:, :, zi].reshape(4 * LY, 128) for zi in range(8)]
        for di, w in enumerate(swap_blocks(v, HX)):
            o_ref[8 * t + di, 0] = w.reshape(2, 2, LY, 128)


def y_forward(me_ref, x_ref, th_ref, tl_ref, *refs):
    o_refs, block_ref, s_refs = refs[:NCOL], refs[NCOL], refs[NCOL + 1 :]
    rows = []
    for zq in range(2):
        x = jnp.concatenate([x_ref[:, 0, r, zq].reshape(GY, 128) for r in range(2)], axis=0)
        rows.append(x.T)
    acc = right(jnp.concatenate(rows, axis=0), ahead(th_ref), ahead(tl_ref), 1)
    for r in range(2):
        for t in range(2):
            s_ref = s_refs[2 * r + t]
            lane = r * 256 + t * 128
            s_ref[...] = acc[:, lane : lane + 128]
            v = []
            for ki in range(4):
                v.append(jnp.concatenate([s_ref[pl.ds(4 * kq + ki, LZ, stride=HX), :] for kq in range(4)], axis=0))
            for ei, w in enumerate(swap_blocks(v, PY)):
                block_ref[4 * t + ei, r] = w.reshape(4, LZ, 128)
    for d in range(NCOL):
        o_refs[d][0] = block_ref[me_ref[0] ^ d]


def z_both(_, me_ref, g_ref, th_ref, tl_ref, bh_ref, bl_ref, *refs):
    x_refs, o_refs, s_ref = refs[:NCOL], refs[NCOL : 2 * NCOL], refs[2 * NCOL]
    nk = x_refs[0].shape[2]
    th, tl = ahead(th_ref), ahead(tl_ref)
    bh, bl = behind(bh_ref), behind(bl_ref)
    spectra = []
    for c in range(3):
        for d in range(NCOL):
            for r in range(2):
                row = pl.multiple_of(r * GZ + (me_ref[0] ^ d) * LZ, LZ)
                for k in range(nk):
                    s_ref[c, pl.ds(row, LZ), k * 128 : (k + 1) * 128] = x_refs[d][c, r, k]
        spectra.append(left(th, tl, s_ref[c], 0))
    for c in range(3):
        pieces = []
        for r in range(2):
            total = None
            for j in range(3):
                term = g_ref[tensor_pairs[c][j]].astype(F32) * spectra[j][r * 256 : (r + 1) * 256]
                total = term if total is None else total + term
            pieces.append(total)
        s_ref[c] = left(bh, bl, jnp.concatenate(pieces, axis=0), 0)
        for d in range(NCOL):
            for r in range(2):
                row = pl.multiple_of(r * GZ + (me_ref[0] ^ d) * LZ, LZ)
                for k in range(nk):
                    o_refs[d][c, r, k] = s_ref[c, pl.ds(row, LZ), k * 128 : (k + 1) * 128]


def y_back(_, me_ref, bh_ref, bl_ref, *refs):
    x_refs, o_ref, block_ref, s_refs = refs[:NCOL], refs[NCOL], refs[NCOL + 1], refs[NCOL + 2 :]
    for d in range(NCOL):
        block_ref[me_ref[0] ^ d] = x_refs[d][0]
    for r in range(2):
        for t in range(2):
            s_ref = s_refs[2 * r + t]
            v = [block_ref[4 * t + ei, r].reshape(4 * LZ, 128) for ei in range(4)]
            for ki, w in enumerate(swap_blocks(v, PY)):
                for kq in range(4):
                    s_ref[pl.ds(4 * kq + ki, LZ, stride=HX), :] = w[kq * LZ : (kq + 1) * LZ]
    x = jnp.concatenate([s_ref[...] for s_ref in s_refs], axis=1)
    acc = left(behind(bh_ref), behind(bl_ref), x, 1)
    for r in range(2):
        for zq in range(2):
            o_ref[:, 0, r, zq] = acc[r * GY : (r + 1) * GY, zq * 128 : (zq + 1) * 128].reshape(NROW, LY, 128)


def put_row(sums, first):
    rows = [jnp.sum(s, axis=0, keepdims=True) for s in sums]
    rows += [jnp.zeros((1, 128), F32)] * (-len(sums) % 8)
    stacked = jnp.concatenate(rows, axis=0)
    total = jnp.sum(stacked, axis=1, keepdims=True)
    row = lax.broadcasted_iota(jnp.int32, stacked.shape, 0)
    lane = lax.broadcasted_iota(jnp.int32, stacked.shape, 1)
    return jnp.sum(jnp.where(lane == row + first, total, 0.0), axis=0, keepdims=True)


def basis_gram(b_ref, o_ref):
    c = pl.program_id(0)
    zeros = tuple(jnp.zeros((8, 128), F32) for _ in PAIRS)

    def body(z, acc):
        for half in range(2):
            b = [b_ref[i // 2, i % 2, 0, z, :, half * 128 : (half + 1) * 128] for i in range(2 * NB)]
            acc = tuple(a + b[i] * b[k] for a, (i, k) in zip(acc, PAIRS))
        return acc

    acc = lax.fori_loop(0, LZ, body, zeros)

    @pl.when(c == 0)
    def _():
        o_ref[...] = jnp.zeros_like(o_ref)

    o_ref[...] += put_row(list(acc), 19)


def x_part(x_ref, ch_ref, cl_ref, sh_ref, sl_ref):
    n = LZ * LY
    planes = []
    for r in range(2):
        tiles = []
        for t in range(2):
            v = [x_ref[8 * t + di, 0, r].reshape(2 * LY, 128) for di in range(8)]
            w = [q.reshape(2, 1, LY, 128) for q in swap_blocks(v, HX)]
            tiles.append(jnp.concatenate(w, axis=1).reshape(n, 128))
        planes.append(jnp.concatenate(tiles, axis=1))
    planes = jnp.concatenate(planes, axis=0)
    cos = right(planes, ch_ref[...], cl_ref[...], 1)
    sin = right(planes, sh_ref[...], sl_ref[...], 1)
    return [(cos[:n] - sin[n:]).reshape(LZ, LY, GX), (cos[n:] + sin[:n]).reshape(LZ, LY, GX)]


def x_back_first(x_ref, ch_ref, cl_ref, sh_ref, sl_ref, u_ref, chi_ref, o_ref):
    chi = chi_ref[...] * SCALING
    for j, part in enumerate(x_part(x_ref, ch_ref, cl_ref, sh_ref, sl_ref)):
        o_ref[j, 0] = u_ref[0, j, 0] - chi * part


def x_back(x_ref, ch_ref, cl_ref, sh_ref, sl_ref, p_ref, b_ref, chi_ref, g_ref, img_ref, all_ref, o_ref):
    c = pl.program_id(0)
    chi = chi_ref[...] * SCALING
    for j, part in enumerate(x_part(x_ref, ch_ref, cl_ref, sh_ref, sl_ref)):
        img_ref[j, 0] = p_ref[j, 0] - chi * part

    def body(z, sums):
        for half in range(2):
            lanes = slice(half * 128, (half + 1) * 128)
            b = [b_ref[i // 2, i % 2, 0, z, :, lanes] for i in range(2 * NB)]
            p = [img_ref[j, 0, z, :, lanes] for j in range(2)]
            terms = [b[i] * p[j] for i in range(2 * NB) for j in range(2)]
            terms += [p[0] * p[0], p[0] * p[1], p[1] * p[1]]
            sums = tuple(a + q for a, q in zip(sums, terms))
        return sums

    sums = lax.fori_loop(0, LZ, body, tuple(jnp.zeros((8, 128), F32) for _ in range(19)))

    @pl.when(c == 0)
    def _():
        o_ref[...] = g_ref[...]

    o_ref[...] += put_row(list(sums), 0)

    @pl.when(c == pl.num_programs(0) - 1)
    def _():
        all_ref[...] = jnp.broadcast_to(o_ref[...], all_ref.shape)


def finish(all_ref, img_ref, b_ref, o_ref, coef_ref, factor_ref, row_ref, s_ref, v_ref):
    @pl.when(pl.program_id(0) == 0)
    def _():
        row_ref[...] = jnp.sum(all_ref[...], axis=0, keepdims=True) / ENTRY
        pltpu.sync_copy(row_ref, s_ref)
        coef = [[s_ref[0, 2 * i + j] for j in range(2)] for i in range(2 * NB)]
        cells = [[None] * (2 * NB) for _ in range(2 * NB)]
        for place, (i, k) in enumerate(PAIRS):
            cells[i][k] = cells[k][i] = s_ref[0, 19 + place]
        mixed = []
        for i in range(2 * NB):
            entry = []
            for j in range(2):
                total = -2.0 * coef[i][j]
                for k in range(2 * NB):
                    total = total + cells[i][k] * coef[k][j]
                entry.append(total)
            mixed.append(entry)
        gram = []
        for place, (j, k) in enumerate(((0, 0), (0, 1), (1, 1))):
            total = s_ref[0, 16 + place]
            for i in range(2 * NB):
                total = total + coef[i][j] * mixed[i][k]
            gram.append(jnp.full((8, 128), total, F32))
        lead = jnp.sqrt(gram[0] + 1e-06)
        cross = gram[1] / lead
        tail = jnp.sqrt(gram[2] - cross * cross + 1e-06)
        v_ref[0] = 1.0 / lead
        v_ref[1] = cross
        v_ref[2] = 1.0 / tail
        for i in range(2 * NB):
            for j in range(2):
                coef_ref[i % 2, j, i // 2] = coef[i][j]
        factor_ref[0, 0] = lead[0, 0]
        factor_ref[0, 1] = cross[0, 0]
        factor_ref[1, 0] = 0.0
        factor_ref[1, 1] = tail[0, 0]

    def body(z, carry):
        for half in range(2):
            lanes = slice(half * 128, (half + 1) * 128)
            p0 = img_ref[0, 0, z, :, lanes]
            p1 = img_ref[1, 0, z, :, lanes]
            for i in range(2 * NB):
                b = b_ref[i // 2, i % 2, 0, z, :, lanes]
                p0 = p0 - s_ref[0, 2 * i] * b
                p1 = p1 - s_ref[0, 2 * i + 1] * b
            p0 = p0 * v_ref[0]
            o_ref[0, 0, z, :, lanes] = p0
            o_ref[1, 0, z, :, lanes] = (p1 - v_ref[1] * p0) * v_ref[2]
        return carry

    lax.fori_loop(0, LZ, body, 0)


def call(body, grid, ins, outs, shapes, scratch=()):
    return pl.pallas_call(
        body,
        grid=grid,
        in_specs=ins,
        out_specs=outs,
        out_shape=shapes,
        scratch_shapes=list(scratch),
        compiler_params=pltpu.CompilerParams(vmem_limit_bytes=VMEM, dimension_semantics=("arbitrary",) * len(grid)),
    )


def whole(shape):
    return pl.BlockSpec(shape, lambda *_: (0,) * len(shape))


def exchange_cols(blocks):
    moved = []
    for d in range(1, NCOL):
        moved.append(lax.ppermute(blocks[d], COL, [(i, i ^ d) for i in range(NCOL)]))
    return [blocks[0]] + moved


def exchange_rows(x):
    return lax.all_to_all(x, ROW, split_axis=0, concat_axis=0, tiled=True)


def per_device(krylov_basis, susceptibility, green_spectra):
    x_tables, side, back = ([jnp.asarray(t) for t in group] for group in tables())
    me = lax.axis_index(COL).astype(jnp.int32).reshape(1)
    row_spec = pl.BlockSpec((NROW, 1, 2, 2, LY, 128), lambda c: (0, c, 0, 0, 0, 0))
    row_shape = jax.ShapeDtypeStruct((NROW, 3, 2, 2, LY, 128), F32)
    col_spec = pl.BlockSpec((1, 2, 4, LZ, 128), lambda c: (c, 0, 0, 0, 0))
    col_shape = jax.ShapeDtypeStruct((3, 2, 4, LZ, 128), F32)
    latest_spec = pl.BlockSpec((1, 2, 1, LZ, LY, GX), lambda c: (NB - 1, 0, c, 0, 0, 0))
    basis_spec = pl.BlockSpec((NB, 2, 1, LZ, LY, GX), lambda c: (0, 0, c, 0, 0, 0))
    image_spec = pl.BlockSpec((2, 1, LZ, LY, GX), lambda c: (0, c, 0, 0, 0))
    image_shape = jax.ShapeDtypeStruct((2, 3, LZ, LY, GX), F32)
    line = jax.ShapeDtypeStruct((1, 128), F32)
    smem = pl.BlockSpec(memory_space=pltpu.SMEM)
    turn = [pltpu.VMEM((NCOL, 2, 4, LZ, 128), F32)] + [pltpu.VMEM((LZ * HX, 128), F32)] * 4
    nk = 2
    z_spec = pl.BlockSpec((3, 2, nk, LZ, 128), lambda k: (0, 0, k, 0, 0))
    green = jnp.swapaxes(green_spectra, 2, 3).reshape(6, 2 * GZ, PX * PY)

    after = pl.BlockSpec(memory_space=pl.ANY)
    table_specs = [[pl.BlockSpec((GX, GX), lambda c, half=half: (0, half))] * 4 for half in range(2)]
    sent = []
    for half in range(2):
        earlier = [green, sent[0]] if half else []
        kernel = call(x_forward, (3,), [after] * len(earlier) + [latest_spec] + table_specs[half], row_spec, row_shape)
        sent.append(kernel(*earlier, krylov_basis, *x_tables))
    rows = [exchange_rows(x) for x in sent]
    own = [
        call(
            y_forward,
            (3,),
            [smem, row_spec, whole(side[0].shape), whole(side[1].shape)],
            [col_spec] * NCOL,
            [col_shape] * NCOL,
            turn,
        )(me, rows[half], *side)
        for half in range(2)
    ]
    cols = [exchange_cols(blocks) for blocks in own]
    mixed = []
    for half in range(2):
        mixed.append(
            call(
                z_both,
                (4 // nk,),
                [
                    after,
                    smem,
                    pl.BlockSpec((6, 2 * GZ, nk * 128), lambda k, half=half: (0, 0, half * (4 // nk) + k)),
                    whole(side[0].shape),
                    whole(side[1].shape),
                    whole(back[0].shape),
                    whole(back[1].shape),
                ]
                + [z_spec] * NCOL,
                [z_spec] * NCOL,
                [col_shape] * NCOL,
                [pltpu.VMEM((3, 2 * GZ, nk * 128), F32)],
            )(own[1 - half][0], me, green, *side, *back, *cols[half])
        )
    cols = [exchange_cols(blocks) for blocks in mixed]
    sent = []
    for half in range(2):
        kernel = call(
            y_back,
            (3,),
            [after, smem, whole(back[0].shape), whole(back[1].shape)] + [col_spec] * NCOL,
            row_spec,
            row_shape,
            turn,
        )
        sent.append(kernel(mixed[1 - half][0], me, *back, *cols[half]))
    arrived = [exchange_rows(x) for x in sent]
    gram_part = call(basis_gram, (3,), [basis_spec], whole((1, 128)), line)(krylov_basis)
    chi_spec = whole((LZ, LY, GX))
    first = call(
        x_back_first, (3,), [row_spec] + table_specs[0] + [latest_spec, chi_spec], image_spec, image_shape
    )(arrived[0], *x_tables, krylov_basis, susceptibility)
    image, everyone = call(
        x_back,
        (3,),
        [row_spec] + table_specs[1] + [image_spec, basis_spec, chi_spec, whole((1, 128))],
        [image_spec, whole((NROW * NCOL, 128))],
        [image_shape, jax.ShapeDtypeStruct((NROW * NCOL, 128), F32)],
        [pltpu.VMEM((1, 128), F32)],
    )(arrived[1], *x_tables, first, krylov_basis, susceptibility, gram_part)
    everyone = everyone.reshape(NROW * NCOL, 1, 128)
    everyone = lax.all_to_all(everyone, ROW_COL, split_axis=0, concat_axis=0, tiled=True)
    next_block, coefficients, factor = call(
        finish,
        (3,),
        [whole((NROW * NCOL, 128)), image_spec, basis_spec],
        [image_spec, smem, smem],
        [image_shape, jax.ShapeDtypeStruct((2, 2, NB), F32), jax.ShapeDtypeStruct((2, 2), F32)],
        [pltpu.VMEM((1, 128), F32), pltpu.SMEM((1, 128), F32), pltpu.VMEM((3, 8, 128), F32)],
    )(everyone.reshape(NROW * NCOL, 128), image, krylov_basis)
    return (jnp.transpose(coefficients, (2, 0, 1)), next_block, factor)


def solution(mesh):
    split_mesh = Mesh(mesh.devices.reshape(4, 4, 4, 2), ("row_0", "row_1", "col_0", "col_1"))

    return jax.shard_map(
        per_device,
        mesh=split_mesh,
        in_specs=(P(None, None, None, COL, ROW, None), P(COL, ROW, None), P(None, None, COL, ROW)),
        out_specs=(P(), P(None, None, COL, ROW, None), P()),
        check_vma=False,
    )
```

```python
import math

import jax
import jax.numpy as jnp
import ml_dtypes
import numpy as np
from jax import lax
from jax.experimental import pallas as pl
from jax.experimental.pallas import tpu as pltpu
from jax.sharding import Mesh
from jax.sharding import PartitionSpec as P

GX = 256
GY = 128
GZ = 128
NB = 4
ROW = ("row_0", "row_1")
COL = ("col_0", "col_1")
ROW_COL = ROW + COL
NROW = 16
NCOL = 8
LZ = GZ // NCOL
LY = GY // NROW
PX = 2 * GX // NROW
HX = PX // 2
PY = 2 * GY // NCOL
F32 = jnp.float32
BF16 = jnp.bfloat16
ENTRY = 3.0 * GX * GY * GZ
SCALING = 1.0 / (8 * GX * GY * GZ)
PAIRS = [(i, k) for i in range(2 * NB) for k in range(i, 2 * NB)]
VMEM = 65024 * 1024
HELD = 57344 * 1024
SMALL = 16 * 1024 * 1024


def split_np(table):
    table = table.astype(np.float32)
    high = table.astype(ml_dtypes.bfloat16)
    low = (table - high.astype(np.float32)).astype(ml_dtypes.bfloat16)
    return [high, low]


def tables():
    kx = np.arange(2 * GX).reshape(NROW, 2, PX // 2).transpose(1, 0, 2).reshape(-1)
    angle = (np.outer(np.arange(GX), kx) % (2 * GX)) * (2.0 * math.pi / (2 * GX))
    x_tables = split_np(np.cos(angle)) + split_np(np.sin(angle))
    angle = (np.outer(np.arange(2 * GY), np.arange(GY)) % (2 * GY)) * (2.0 * math.pi / (2 * GY))
    side = np.concatenate([np.cos(angle), np.sin(angle)], axis=0)
    return x_tables, split_np(side)


def split(x):
    high = x.astype(BF16)
    low = (x - high.astype(F32)).astype(BF16)
    return high, low


def dot(a, b, ca, cb):
    return lax.dot_general(a, b, (((ca,), (cb,)), ((), ())), preferred_element_type=F32)


def ahead(ref):
    c, s = ref[:256], ref[256:]
    return jnp.concatenate([jnp.concatenate([c, s], axis=1), jnp.concatenate([-s, c], axis=1)], axis=0)


def behind(ref):
    c, s = ref[:, :256], ref[:, 256:]
    return jnp.concatenate([jnp.concatenate([c, -s], axis=1), jnp.concatenate([s, c], axis=1)], axis=0)


def left(th, tl, x, cb):
    h, l = split(x)
    n = th.shape[0]
    wide = dot(jnp.concatenate([th, tl], axis=0), h, 1, cb)
    return wide[:n] + (wide[n:] + dot(th, l, 1, cb))


def right(x, th, tl, cb):
    h, l = split(x)
    n = x.shape[0]
    wide = dot(jnp.concatenate([h, l], axis=0), th, 1, cb)
    return wide[:n] + (wide[n:] + dot(h, tl, 1, cb))


def swap_blocks(v, width):
    v = list(v)
    block = lax.broadcasted_iota(jnp.int32, v[0].shape, 1) // width
    step = len(v) // 2
    while step:
        keep = (block & step) == 0
        for i in range(len(v)):
            if i & step == 0:
                p, q = v[i], v[i + step]
                v[i] = jnp.where(keep, p, pltpu.roll(q, step * width, 1))
                v[i + step] = jnp.where(keep, pltpu.roll(p, 128 - step * width, 1), q)
        step //= 2
    return v


def x_forward(*refs):
    u_ref, ch_ref, cl_ref, sh_ref, sl_ref, o_ref = refs[-6:]
    n = LZ * LY
    u = jnp.concatenate([u_ref[0, 0, 0].reshape(n, GX), u_ref[0, 1, 0].reshape(n, GX)], axis=0)
    c = right(u, ch_ref[...], cl_ref[...], 0)
    s = right(u, sh_ref[...], sl_ref[...], 0)
    acc = jnp.concatenate([c[:n] + s[n:], c[n:] - s[:n]], axis=0)
    acc = acc.reshape(2, 2, 8, LY, GX)
    for t in range(2):
        part = acc[..., t * 128 : (t + 1) * 128]
        v = [part[:, :, zi].reshape(4 * LY, 128) for zi in range(8)]
        for di, w in enumerate(swap_blocks(v, HX)):
            o_ref[8 * t + di, 0] = w.reshape(2, 2, LY, 128)


def y_forward(me_ref, x_ref, th_ref, tl_ref, *refs):
    o_refs, block_ref, s_refs = refs[:NCOL], refs[NCOL], refs[NCOL + 1 :]
    rows = []
    for zq in range(2):
        x = jnp.concatenate([x_ref[:, 0, r, zq].reshape(GY, 128) for r in range(2)], axis=0)
        rows.append(x.T)
    acc = right(jnp.concatenate(rows, axis=0), ahead(th_ref), ahead(tl_ref), 1)
    for r in range(2):
        for t in range(2):
            s_ref = s_refs[2 * r + t]
            lane = r * 256 + t * 128
            s_ref[...] = acc[:, lane : lane + 128]
            v = []
            for ki in range(4):
                v.append(jnp.concatenate([s_ref[pl.ds(4 * kq + ki, LZ, stride=HX), :] for kq in range(4)], axis=0))
            for ei, w in enumerate(swap_blocks(v, PY)):
                block_ref[4 * t + ei, r] = w.reshape(4, LZ, 128)
    for d in range(NCOL):
        o_refs[d][0] = block_ref[me_ref[0] ^ d]


def z_both(_, me_ref, g_ref, th_ref, tl_ref, bh_ref, bl_ref, *refs):
    x_refs, o_refs, s_ref, f_ref = refs[:NCOL], refs[NCOL : 2 * NCOL], refs[2 * NCOL], refs[2 * NCOL + 1]
    nk = x_refs[0].shape[2]

    def place(d, r):
        return pl.ds(pl.multiple_of(r * GZ + (me_ref[0] ^ d) * LZ, LZ), LZ)

    def there(c, carry):
        for d in range(NCOL):
            for r in range(2):
                for k in range(nk):
                    s_ref[c, place(d, r), k * 128 : (k + 1) * 128] = x_refs[d][c, r, k]
        f_ref[c] = left(ahead(th_ref), ahead(tl_ref), s_ref[c], 0)
        return carry

    def again(c, carry):
        pieces = []
        for r in range(2):
            total = None
            for j in range(3):
                entry = jnp.where(c == j, c, c + j + 2)
                term = g_ref[entry].astype(F32) * f_ref[j, r * 256 : (r + 1) * 256]
                total = term if total is None else total + term
            pieces.append(total)
        s_ref[c] = left(behind(bh_ref), behind(bl_ref), jnp.concatenate(pieces, axis=0), 0)
        for d in range(NCOL):
            for r in range(2):
                for k in range(nk):
                    o_refs[d][c, r, k] = s_ref[c, place(d, r), k * 128 : (k + 1) * 128]
        return carry

    lax.fori_loop(0, 3, there, 0)
    lax.fori_loop(0, 3, again, 0)


def y_back(_, me_ref, bh_ref, bl_ref, *refs):
    x_refs, o_ref, block_ref, s_refs = refs[:NCOL], refs[NCOL], refs[NCOL + 1], refs[NCOL + 2 :]
    for d in range(NCOL):
        block_ref[me_ref[0] ^ d] = x_refs[d][0]
    for r in range(2):
        for t in range(2):
            s_ref = s_refs[2 * r + t]
            v = [block_ref[4 * t + ei, r].reshape(4 * LZ, 128) for ei in range(4)]
            for ki, w in enumerate(swap_blocks(v, PY)):
                for kq in range(4):
                    s_ref[pl.ds(4 * kq + ki, LZ, stride=HX), :] = w[kq * LZ : (kq + 1) * LZ]
    x = jnp.concatenate([s_ref[...] for s_ref in s_refs], axis=1)
    acc = left(behind(bh_ref), behind(bl_ref), x, 1)
    for r in range(2):
        for zq in range(2):
            o_ref[:, 0, r, zq] = acc[r * GY : (r + 1) * GY, zq * 128 : (zq + 1) * 128].reshape(NROW, LY, 128)


def put_row(sums, first):
    rows = [jnp.sum(s, axis=0, keepdims=True) for s in sums]
    rows += [jnp.zeros((1, 128), F32)] * (-len(sums) % 8)
    stacked = jnp.concatenate(rows, axis=0)
    total = jnp.sum(stacked, axis=1, keepdims=True)
    row = lax.broadcasted_iota(jnp.int32, stacked.shape, 0)
    lane = lax.broadcasted_iota(jnp.int32, stacked.shape, 1)
    return jnp.sum(jnp.where(lane == row + first, total, 0.0), axis=0, keepdims=True)


def basis_gram(b_ref, o_ref):
    c = pl.program_id(0)
    zeros = tuple(jnp.zeros((8, 128), F32) for _ in PAIRS)

    def body(z, acc):
        for half in range(2):
            b = [b_ref[i // 2, i % 2, 0, z, :, half * 128 : (half + 1) * 128] for i in range(2 * NB)]
            acc = tuple(a + b[i] * b[k] for a, (i, k) in zip(acc, PAIRS))
        return acc

    acc = lax.fori_loop(0, LZ, body, zeros)

    @pl.when(c == 0)
    def _():
        o_ref[...] = jnp.zeros_like(o_ref)

    o_ref[...] += put_row(list(acc), 19)


def x_part(x_ref, ch_ref, cl_ref, sh_ref, sl_ref):
    n = LZ * LY
    planes = []
    for r in range(2):
        tiles = []
        for t in range(2):
            v = [x_ref[8 * t + di, 0, r].reshape(2 * LY, 128) for di in range(8)]
            w = [q.reshape(2, 1, LY, 128) for q in swap_blocks(v, HX)]
            tiles.append(jnp.concatenate(w, axis=1).reshape(n, 128))
        planes.append(jnp.concatenate(tiles, axis=1))
    planes = jnp.concatenate(planes, axis=0)
    cos = right(planes, ch_ref[...], cl_ref[...], 1)
    sin = right(planes, sh_ref[...], sl_ref[...], 1)
    return [(cos[:n] - sin[n:]).reshape(LZ, LY, GX), (cos[n:] + sin[:n]).reshape(LZ, LY, GX)]


def x_back_first(x_ref, ch_ref, cl_ref, sh_ref, sl_ref, u_ref, chi_ref, o_ref):
    chi = chi_ref[...] * SCALING
    for j, part in enumerate(x_part(x_ref, ch_ref, cl_ref, sh_ref, sl_ref)):
        o_ref[j, 0] = u_ref[0, j, 0] - chi * part


def x_back(x_ref, ch_ref, cl_ref, sh_ref, sl_ref, p_ref, b_ref, chi_ref, g_ref, img_ref, all_ref, o_ref):
    c = pl.program_id(0)
    chi = chi_ref[...] * SCALING
    for j, part in enumerate(x_part(x_ref, ch_ref, cl_ref, sh_ref, sl_ref)):
        img_ref[j, 0] = p_ref[j, 0] - chi * part

    def body(z, sums):
        for half in range(2):
            lanes = slice(half * 128, (half + 1) * 128)
            b = [b_ref[i // 2, i % 2, 0, z, :, lanes] for i in range(2 * NB)]
            p = [img_ref[j, 0, z, :, lanes] for j in range(2)]
            terms = [b[i] * p[j] for i in range(2 * NB) for j in range(2)]
            terms += [p[0] * p[0], p[0] * p[1], p[1] * p[1]]
            sums = tuple(a + q for a, q in zip(sums, terms))
        return sums

    sums = lax.fori_loop(0, LZ, body, tuple(jnp.zeros((8, 128), F32) for _ in range(19)))

    @pl.when(c == 0)
    def _():
        o_ref[...] = g_ref[...]

    o_ref[...] += put_row(list(sums), 0)

    @pl.when(c == pl.num_programs(0) - 1)
    def _():
        all_ref[...] = jnp.broadcast_to(o_ref[...], all_ref.shape)


def finish(all_ref, img_ref, b_ref, o_ref, coef_ref, factor_ref, row_ref, s_ref, v_ref):
    @pl.when(pl.program_id(0) == 0)
    def _():
        row_ref[...] = jnp.sum(all_ref[...], axis=0, keepdims=True) / ENTRY
        pltpu.sync_copy(row_ref, s_ref)
        coef = [[s_ref[0, 2 * i + j] for j in range(2)] for i in range(2 * NB)]
        cells = [[None] * (2 * NB) for _ in range(2 * NB)]
        for place, (i, k) in enumerate(PAIRS):
            cells[i][k] = cells[k][i] = s_ref[0, 19 + place]
        mixed = []
        for i in range(2 * NB):
            entry = []
            for j in range(2):
                total = -2.0 * coef[i][j]
                for k in range(2 * NB):
                    total = total + cells[i][k] * coef[k][j]
                entry.append(total)
            mixed.append(entry)
        gram = []
        for place, (j, k) in enumerate(((0, 0), (0, 1), (1, 1))):
            total = s_ref[0, 16 + place]
            for i in range(2 * NB):
                total = total + coef[i][j] * mixed[i][k]
            gram.append(jnp.full((8, 128), total, F32))
        lead = jnp.sqrt(gram[0] + 1e-06)
        cross = gram[1] / lead
        tail = jnp.sqrt(gram[2] - cross * cross + 1e-06)
        v_ref[0] = 1.0 / lead
        v_ref[1] = cross
        v_ref[2] = 1.0 / tail
        for i in range(2 * NB):
            for j in range(2):
                coef_ref[i % 2, j, i // 2] = coef[i][j]
        factor_ref[0, 0] = lead[0, 0]
        factor_ref[0, 1] = cross[0, 0]
        factor_ref[1, 0] = 0.0
        factor_ref[1, 1] = tail[0, 0]

    def body(z, carry):
        for half in range(2):
            lanes = slice(half * 128, (half + 1) * 128)
            p0 = img_ref[0, 0, z, :, lanes]
            p1 = img_ref[1, 0, z, :, lanes]
            for i in range(2 * NB):
                b = b_ref[i // 2, i % 2, 0, z, :, lanes]
                p0 = p0 - s_ref[0, 2 * i] * b
                p1 = p1 - s_ref[0, 2 * i + 1] * b
            p0 = p0 * v_ref[0]
            o_ref[0, 0, z, :, lanes] = p0
            o_ref[1, 0, z, :, lanes] = (p1 - v_ref[1] * p0) * v_ref[2]
        return carry

    lax.fori_loop(0, LZ, body, 0)


def call(body, grid, ins, outs, shapes, scratch=(), grant=VMEM):
    return pl.pallas_call(
        body,
        grid=grid,
        in_specs=ins,
        out_specs=outs,
        out_shape=shapes,
        scratch_shapes=list(scratch),
        compiler_params=pltpu.CompilerParams(vmem_limit_bytes=grant, dimension_semantics=("arbitrary",) * len(grid)),
    )


def whole(shape):
    return pl.BlockSpec(shape, lambda *_: (0,) * len(shape))


def exchange_cols(blocks):
    moved = []
    for d in range(1, NCOL):
        moved.append(lax.ppermute(blocks[d], COL, [(i, i ^ d) for i in range(NCOL)]))
    return [blocks[0]] + moved


def exchange_rows(x):
    return lax.all_to_all(x, ROW, split_axis=0, concat_axis=0, tiled=True)


def per_device(krylov_basis, susceptibility, green_spectra):
    x_tables, side = ([jnp.asarray(t) for t in group] for group in tables())
    me = lax.axis_index(COL).astype(jnp.int32).reshape(1)
    row_spec = pl.BlockSpec((NROW, 1, 2, 2, LY, 128), lambda c: (0, c, 0, 0, 0, 0))
    row_shape = jax.ShapeDtypeStruct((NROW, 3, 2, 2, LY, 128), F32)
    col_spec = pl.BlockSpec((1, 2, 4, LZ, 128), lambda c: (c, 0, 0, 0, 0))
    col_shape = jax.ShapeDtypeStruct((3, 2, 4, LZ, 128), F32)
    latest_spec = pl.BlockSpec((1, 2, 1, LZ, LY, GX), lambda c: (NB - 1, 0, c, 0, 0, 0))
    basis_spec = pl.BlockSpec((NB, 2, 1, LZ, LY, GX), lambda c: (0, 0, c, 0, 0, 0))
    image_spec = pl.BlockSpec((2, 1, LZ, LY, GX), lambda c: (0, c, 0, 0, 0))
    image_shape = jax.ShapeDtypeStruct((2, 3, LZ, LY, GX), F32)
    line = jax.ShapeDtypeStruct((1, 128), F32)
    smem = pl.BlockSpec(memory_space=pltpu.SMEM)
    turn = [pltpu.VMEM((NCOL, 2, 4, LZ, 128), F32)] + [pltpu.VMEM((LZ * HX, 128), F32)] * 4
    nk = 2
    z_spec = pl.BlockSpec((3, 2, nk, LZ, 128), lambda k: (0, 0, k, 0, 0))
    green = jnp.swapaxes(green_spectra, 2, 3).reshape(6, 2 * GZ, PX * PY)

    after = pl.BlockSpec(memory_space=pl.ANY)
    table_specs = [[pl.BlockSpec((GX, GX), lambda c, half=half: (0, half))] * 4 for half in range(2)]
    sent = []
    for half in range(2):
        earlier = [green, sent[0]] if half else []
        kernel = call(x_forward, (3,), [after] * len(earlier) + [latest_spec] + table_specs[half], row_spec, row_shape)
        sent.append(kernel(*earlier, krylov_basis, *x_tables))
    rows = [exchange_rows(x) for x in sent]
    back = [t.T for t in lax.optimization_barrier((*side, sent[0]))[:2]]
    own = [
        call(
            y_forward,
            (3,),
            [smem, row_spec, whole(side[0].shape), whole(side[1].shape)],
            [col_spec] * NCOL,
            [col_shape] * NCOL,
            turn,
        )(me, rows[half], *side)
        for half in range(2)
    ]
    cols = [exchange_cols(blocks) for blocks in own]
    mixed = []
    for half in range(2):
        mixed.append(
            call(
                z_both,
                (4 // nk,),
                [
                    after,
                    smem,
                    pl.BlockSpec((6, 2 * GZ, nk * 128), lambda k, half=half: (0, 0, half * (4 // nk) + k)),
                    whole(side[0].shape),
                    whole(side[1].shape),
                    whole(back[0].shape),
                    whole(back[1].shape),
                ]
                + [z_spec] * NCOL,
                [z_spec] * NCOL,
                [col_shape] * NCOL,
                [pltpu.VMEM((3, 2 * GZ, nk * 128), F32), pltpu.VMEM((3, 4 * GZ, nk * 128), F32)],
            )(own[1 - half][0], me, green, *side, *back, *cols[half])
        )
    cols = [exchange_cols(blocks) for blocks in mixed]
    sent = []
    for half in range(2):
        kernel = call(
            y_back,
            (3,),
            [after, smem, whole(back[0].shape), whole(back[1].shape)] + [col_spec] * NCOL,
            row_spec,
            row_shape,
            turn,
        )
        sent.append(kernel(mixed[1 - half][0], me, *back, *cols[half]))
    arrived = [exchange_rows(x) for x in sent]
    gram_part = call(basis_gram, (3,), [basis_spec], whole((1, 128)), line)(krylov_basis)
    chi_spec = whole((LZ, LY, GX))
    first = call(
        x_back_first, (3,), [row_spec] + table_specs[0] + [latest_spec, chi_spec], image_spec, image_shape
    )(arrived[0], *x_tables, krylov_basis, susceptibility)
    image, everyone = call(
        x_back,
        (3,),
        [row_spec] + table_specs[1] + [image_spec, basis_spec, chi_spec, whole((1, 128))],
        [image_spec, whole((NROW * NCOL, 128))],
        [image_shape, jax.ShapeDtypeStruct((NROW * NCOL, 128), F32)],
        [pltpu.VMEM((1, 128), F32)],
        HELD,
    )(arrived[1], *x_tables, first, krylov_basis, susceptibility, gram_part)
    everyone = everyone.reshape(NROW * NCOL, 1, 128)
    everyone = lax.all_to_all(everyone, ROW_COL, split_axis=0, concat_axis=0, tiled=True)
    next_block, coefficients, factor = call(
        finish,
        (3,),
        [whole((NROW * NCOL, 128)), image_spec, basis_spec],
        [image_spec, smem, smem],
        [image_shape, jax.ShapeDtypeStruct((2, 2, NB), F32), jax.ShapeDtypeStruct((2, 2), F32)],
        [pltpu.VMEM((1, 128), F32), pltpu.SMEM((1, 128), F32), pltpu.VMEM((3, 8, 128), F32)],
        SMALL,
    )(everyone.reshape(NROW * NCOL, 128), image, krylov_basis)
    return (jnp.transpose(coefficients, (2, 0, 1)), next_block, factor)


def solution(mesh):
    split_mesh = Mesh(mesh.devices.reshape(4, 4, 4, 2), ("row_0", "row_1", "col_0", "col_1"))

    return jax.shard_map(
        per_device,
        mesh=split_mesh,
        in_specs=(P(None, None, None, COL, ROW, None), P(COL, ROW, None), P(None, None, COL, ROW)),
        out_specs=(P(), P(None, None, COL, ROW, None), P()),
        check_vma=False,
    )
```

```python
import math

import jax
import jax.numpy as jnp
import ml_dtypes
import numpy as np
from jax import lax
from jax.experimental import pallas as pl
from jax.experimental.pallas import tpu as pltpu
from jax.sharding import Mesh
from jax.sharding import PartitionSpec as P

GX = 256
GY = 128
GZ = 128
NB = 4
ROW = ("row_0", "row_1")
COL = ("col_0", "col_1")
ROW_COL = ROW + COL
NROW = 16
NCOL = 8
LZ = GZ // NCOL
LY = GY // NROW
PX = 2 * GX // NROW
HX = PX // 2
PY = 2 * GY // NCOL
F32 = jnp.float32
BF16 = jnp.bfloat16
ENTRY = 3.0 * GX * GY * GZ
SCALING = 1.0 / (8 * GX * GY * GZ)
PAIRS = [(i, k) for i in range(2 * NB) for k in range(i, 2 * NB)]
VMEM = 65024 * 1024
HELD = 40 * 1024 * 1024
ROOMY = 36
SMALL = 16 * 1024 * 1024


def split_np(table):
    table = table.astype(np.float32)
    high = table.astype(ml_dtypes.bfloat16)
    low = (table - high.astype(np.float32)).astype(ml_dtypes.bfloat16)
    return [high, low]


def tables():
    kx = np.arange(2 * GX).reshape(NROW, 2, PX // 2).transpose(1, 0, 2).reshape(-1)
    angle = (np.outer(np.arange(GX), kx) % (2 * GX)) * (2.0 * math.pi / (2 * GX))
    x_tables = split_np(np.cos(angle)) + split_np(np.sin(angle))
    angle = (np.outer(np.arange(2 * GY), np.arange(GY)) % (2 * GY)) * (2.0 * math.pi / (2 * GY))
    side = np.concatenate([np.cos(angle), np.sin(angle)], axis=0)
    return x_tables, split_np(side)


def split(x):
    high = x.astype(BF16)
    low = (x - high.astype(F32)).astype(BF16)
    return high, low


def dot(a, b, ca, cb):
    return lax.dot_general(a, b, (((ca,), (cb,)), ((), ())), preferred_element_type=F32)


def ahead(ref):
    c, s = ref[:256], ref[256:]
    return jnp.concatenate([jnp.concatenate([c, s], axis=1), jnp.concatenate([-s, c], axis=1)], axis=0)


def behind(ref):
    c, s = ref[:, :256], ref[:, 256:]
    return jnp.concatenate([jnp.concatenate([c, -s], axis=1), jnp.concatenate([s, c], axis=1)], axis=0)


def left(th, tl, x, cb):
    h, l = split(x)
    n = th.shape[0]
    wide = dot(jnp.concatenate([th, tl], axis=0), h, 1, cb)
    return wide[:n] + (wide[n:] + dot(th, l, 1, cb))


def right(x, th, tl, cb):
    h, l = split(x)
    n = x.shape[0]
    wide = dot(jnp.concatenate([h, l], axis=0), th, 1, cb)
    return wide[:n] + (wide[n:] + dot(h, tl, 1, cb))


def swap_blocks(v, width):
    v = list(v)
    block = lax.broadcasted_iota(jnp.int32, v[0].shape, 1) // width
    step = len(v) // 2
    while step:
        keep = (block & step) == 0
        for i in range(len(v)):
            if i & step == 0:
                p, q = v[i], v[i + step]
                v[i] = jnp.where(keep, p, pltpu.roll(q, step * width, 1))
                v[i + step] = jnp.where(keep, pltpu.roll(p, 128 - step * width, 1), q)
        step //= 2
    return v


def x_forward(*refs):
    u_ref, ch_ref, cl_ref, sh_ref, sl_ref, o_ref = refs[-6:]
    n = LZ * LY
    u = jnp.concatenate([u_ref[0, 0, 0].reshape(n, GX), u_ref[0, 1, 0].reshape(n, GX)], axis=0)
    c = right(u, ch_ref[...], cl_ref[...], 0)
    s = right(u, sh_ref[...], sl_ref[...], 0)
    acc = jnp.concatenate([c[:n] + s[n:], c[n:] - s[:n]], axis=0)
    acc = acc.reshape(2, 2, 8, LY, GX)
    for t in range(2):
        part = acc[..., t * 128 : (t + 1) * 128]
        v = [part[:, :, zi].reshape(4 * LY, 128) for zi in range(8)]
        for di, w in enumerate(swap_blocks(v, HX)):
            o_ref[8 * t + di, 0] = w.reshape(2, 2, LY, 128)


def y_forward(me_ref, x_ref, th_ref, tl_ref, *refs):
    o_refs, block_ref, s_refs = refs[:NCOL], refs[NCOL], refs[NCOL + 1 :]
    rows = []
    for zq in range(2):
        x = jnp.concatenate([x_ref[:, 0, r, zq].reshape(GY, 128) for r in range(2)], axis=0)
        rows.append(x.T)
    acc = right(jnp.concatenate(rows, axis=0), ahead(th_ref), ahead(tl_ref), 1)
    for r in range(2):
        for t in range(2):
            s_ref = s_refs[2 * r + t]
            lane = r * 256 + t * 128
            s_ref[...] = acc[:, lane : lane + 128]
            v = []
            for ki in range(4):
                v.append(jnp.concatenate([s_ref[pl.ds(4 * kq + ki, LZ, stride=HX), :] for kq in range(4)], axis=0))
            for ei, w in enumerate(swap_blocks(v, PY)):
                block_ref[4 * t + ei, r] = w.reshape(4, LZ, 128)
    for d in range(NCOL):
        o_refs[d][0] = block_ref[me_ref[0] ^ d]


def z_both(_, me_ref, g_ref, th_ref, tl_ref, bh_ref, bl_ref, *refs):
    x_refs, o_refs, s_ref, f_ref = refs[:NCOL], refs[NCOL : 2 * NCOL], refs[2 * NCOL], refs[2 * NCOL + 1]
    nk = x_refs[0].shape[2]

    def place(d, r):
        return pl.ds(pl.multiple_of(r * GZ + (me_ref[0] ^ d) * LZ, LZ), LZ)

    def there(c, carry):
        for d in range(NCOL):
            for r in range(2):
                for k in range(nk):
                    s_ref[c, place(d, r), k * 128 : (k + 1) * 128] = x_refs[d][c, r, k]
        f_ref[c] = left(ahead(th_ref), ahead(tl_ref), s_ref[c], 0)
        return carry

    def again(c, carry):
        pieces = []
        for r in range(2):
            total = None
            for j in range(3):
                entry = jnp.where(c == j, c, c + j + 2)
                term = g_ref[entry].astype(F32) * f_ref[j, r * 256 : (r + 1) * 256]
                total = term if total is None else total + term
            pieces.append(total)
        s_ref[c] = left(behind(bh_ref), behind(bl_ref), jnp.concatenate(pieces, axis=0), 0)
        for d in range(NCOL):
            for r in range(2):
                for k in range(nk):
                    o_refs[d][c, r, k] = s_ref[c, place(d, r), k * 128 : (k + 1) * 128]
        return carry

    lax.fori_loop(0, 3, there, 0)
    lax.fori_loop(0, 3, again, 0)


def y_back(_, me_ref, bh_ref, bl_ref, *refs):
    x_refs, o_ref, block_ref, s_refs = refs[:NCOL], refs[NCOL], refs[NCOL + 1], refs[NCOL + 2 :]
    for d in range(NCOL):
        block_ref[me_ref[0] ^ d] = x_refs[d][0]
    for r in range(2):
        for t in range(2):
            s_ref = s_refs[2 * r + t]
            v = [block_ref[4 * t + ei, r].reshape(4 * LZ, 128) for ei in range(4)]
            for ki, w in enumerate(swap_blocks(v, PY)):
                for kq in range(4):
                    s_ref[pl.ds(4 * kq + ki, LZ, stride=HX), :] = w[kq * LZ : (kq + 1) * LZ]
    x = jnp.concatenate([s_ref[...] for s_ref in s_refs], axis=1)
    acc = left(behind(bh_ref), behind(bl_ref), x, 1)
    for r in range(2):
        for zq in range(2):
            o_ref[:, 0, r, zq] = acc[r * GY : (r + 1) * GY, zq * 128 : (zq + 1) * 128].reshape(NROW, LY, 128)


def put_row(sums, first):
    rows = [jnp.sum(s, axis=0, keepdims=True) for s in sums]
    rows += [jnp.zeros((1, 128), F32)] * (-len(sums) % 8)
    stacked = jnp.concatenate(rows, axis=0)
    total = jnp.sum(stacked, axis=1, keepdims=True)
    row = lax.broadcasted_iota(jnp.int32, stacked.shape, 0)
    lane = lax.broadcasted_iota(jnp.int32, stacked.shape, 1)
    return jnp.sum(jnp.where(lane == row + first, total, 0.0), axis=0, keepdims=True)


def basis_gram(b_ref, o_ref):
    c = pl.program_id(0)
    zeros = tuple(jnp.zeros((8, 128), F32) for _ in PAIRS)

    def body(z, acc):
        for half in range(2):
            b = [b_ref[i // 2, i % 2, 0, z, :, half * 128 : (half + 1) * 128] for i in range(2 * NB)]
            acc = tuple(a + b[i] * b[k] for a, (i, k) in zip(acc, PAIRS))
        return acc

    acc = lax.fori_loop(0, LZ, body, zeros)

    @pl.when(c == 0)
    def _():
        o_ref[...] = jnp.zeros_like(o_ref)

    o_ref[...] += put_row(list(acc), 19)


def x_part(x_ref, ch_ref, cl_ref, sh_ref, sl_ref):
    n = LZ * LY
    planes = []
    for r in range(2):
        tiles = []
        for t in range(2):
            v = [x_ref[8 * t + di, 0, r].reshape(2 * LY, 128) for di in range(8)]
            w = [q.reshape(2, 1, LY, 128) for q in swap_blocks(v, HX)]
            tiles.append(jnp.concatenate(w, axis=1).reshape(n, 128))
        planes.append(jnp.concatenate(tiles, axis=1))
    planes = jnp.concatenate(planes, axis=0)
    cos = right(planes, ch_ref[...], cl_ref[...], 1)
    sin = right(planes, sh_ref[...], sl_ref[...], 1)
    return [(cos[:n] - sin[n:]).reshape(LZ, LY, GX), (cos[n:] + sin[:n]).reshape(LZ, LY, GX)]


def x_back_first(x_ref, ch_ref, cl_ref, sh_ref, sl_ref, *refs):
    others, (u_ref, chi_ref, o_ref, t_ref) = refs[:4], refs[4:]
    for place, other in enumerate(others):
        t_ref[place] = other[...]
    chi = chi_ref[...] * SCALING
    for j, part in enumerate(x_part(x_ref, ch_ref, cl_ref, sh_ref, sl_ref)):
        o_ref[j, 0] = u_ref[0, j, 0] - chi * part


def x_back(x_ref, t_ref, p_ref, b_ref, chi_ref, g_ref, img_ref, all_ref, o_ref):
    c = pl.program_id(0)
    chi = chi_ref[...] * SCALING
    for j, part in enumerate(x_part(x_ref, *(t_ref.at[place] for place in range(4)))):
        img_ref[j, 0] = p_ref[j, 0] - chi * part

    def body(z, sums):
        for half in range(2):
            lanes = slice(half * 128, (half + 1) * 128)
            b = [b_ref[i // 2, i % 2, 0, z, :, lanes] for i in range(2 * NB)]
            p = [img_ref[j, 0, z, :, lanes] for j in range(2)]
            terms = [b[i] * p[j] for i in range(2 * NB) for j in range(2)]
            terms += [p[0] * p[0], p[0] * p[1], p[1] * p[1]]
            sums = tuple(a + q for a, q in zip(sums, terms))
        return sums

    sums = lax.fori_loop(0, LZ, body, tuple(jnp.zeros((8, 128), F32) for _ in range(19)))

    @pl.when(c == 0)
    def _():
        o_ref[...] = g_ref[...]

    o_ref[...] += put_row(list(sums), 0)

    @pl.when(c == pl.num_programs(0) - 1)
    def _():
        all_ref[...] = jnp.broadcast_to(o_ref[...], all_ref.shape)


def finish(all_ref, img_ref, b_ref, o_ref, coef_ref, factor_ref, row_ref, s_ref, v_ref):
    @pl.when(pl.program_id(0) == 0)
    def _():
        row_ref[...] = jnp.sum(all_ref[...], axis=0, keepdims=True) / ENTRY
        pltpu.sync_copy(row_ref, s_ref)
        coef = [[s_ref[0, 2 * i + j] for j in range(2)] for i in range(2 * NB)]
        cells = [[None] * (2 * NB) for _ in range(2 * NB)]
        for place, (i, k) in enumerate(PAIRS):
            cells[i][k] = cells[k][i] = s_ref[0, 19 + place]
        mixed = []
        for i in range(2 * NB):
            entry = []
            for j in range(2):
                total = -2.0 * coef[i][j]
                for k in range(2 * NB):
                    total = total + cells[i][k] * coef[k][j]
                entry.append(total)
            mixed.append(entry)
        gram = []
        for place, (j, k) in enumerate(((0, 0), (0, 1), (1, 1))):
            total = s_ref[0, 16 + place]
            for i in range(2 * NB):
                total = total + coef[i][j] * mixed[i][k]
            gram.append(jnp.full((8, 128), total, F32))
        lead = jnp.sqrt(gram[0] + 1e-06)
        cross = gram[1] / lead
        tail = jnp.sqrt(gram[2] - cross * cross + 1e-06)
        v_ref[0] = 1.0 / lead
        v_ref[1] = cross
        v_ref[2] = 1.0 / tail
        for i in range(2 * NB):
            for j in range(2):
                coef_ref[i % 2, j, i // 2] = coef[i][j]
        factor_ref[0, 0] = lead[0, 0]
        factor_ref[0, 1] = cross[0, 0]
        factor_ref[1, 0] = 0.0
        factor_ref[1, 1] = tail[0, 0]

    def body(z, carry):
        for half in range(2):
            lanes = slice(half * 128, (half + 1) * 128)
            p0 = img_ref[0, 0, z, :, lanes]
            p1 = img_ref[1, 0, z, :, lanes]
            for i in range(2 * NB):
                b = b_ref[i // 2, i % 2, 0, z, :, lanes]
                p0 = p0 - s_ref[0, 2 * i] * b
                p1 = p1 - s_ref[0, 2 * i + 1] * b
            p0 = p0 * v_ref[0]
            o_ref[0, 0, z, :, lanes] = p0
            o_ref[1, 0, z, :, lanes] = (p1 - v_ref[1] * p0) * v_ref[2]
        return carry

    lax.fori_loop(0, LZ, body, 0)


def call(body, grid, ins, outs, shapes, scratch=(), grant=VMEM):
    return pl.pallas_call(
        body,
        grid=grid,
        in_specs=ins,
        out_specs=outs,
        out_shape=shapes,
        scratch_shapes=list(scratch),
        compiler_params=pltpu.CompilerParams(vmem_limit_bytes=grant, dimension_semantics=("arbitrary",) * len(grid)),
    )


def whole(shape):
    return pl.BlockSpec(shape, lambda *_: (0,) * len(shape))


def exchange_cols(blocks):
    moved = []
    for d in range(1, NCOL):
        moved.append(lax.ppermute(blocks[d], COL, [(i, i ^ d) for i in range(NCOL)]))
    return [blocks[0]] + moved


def exchange_rows(x):
    return lax.all_to_all(x, ROW, split_axis=0, concat_axis=0, tiled=True)


def per_device(krylov_basis, susceptibility, green_spectra):
    x_tables, side = ([jnp.asarray(t) for t in group] for group in tables())
    me = lax.axis_index(COL).astype(jnp.int32).reshape(1)
    row_spec = pl.BlockSpec((NROW, 1, 2, 2, LY, 128), lambda c: (0, c, 0, 0, 0, 0))
    row_shape = jax.ShapeDtypeStruct((NROW, 3, 2, 2, LY, 128), F32)
    col_spec = pl.BlockSpec((1, 2, 4, LZ, 128), lambda c: (c, 0, 0, 0, 0))
    col_shape = jax.ShapeDtypeStruct((3, 2, 4, LZ, 128), F32)
    latest_spec = pl.BlockSpec((1, 2, 1, LZ, LY, GX), lambda c: (NB - 1, 0, c, 0, 0, 0))
    basis_spec = pl.BlockSpec((NB, 2, 1, LZ, LY, GX), lambda c: (0, 0, c, 0, 0, 0))
    image_spec = pl.BlockSpec((2, 1, LZ, LY, GX), lambda c: (0, c, 0, 0, 0))
    image_shape = jax.ShapeDtypeStruct((2, 3, LZ, LY, GX), F32)
    line = jax.ShapeDtypeStruct((1, 128), F32)
    smem = pl.BlockSpec(memory_space=pltpu.SMEM)
    turn = [pltpu.VMEM((NCOL, 2, 4, LZ, 128), F32)] + [pltpu.VMEM((LZ * HX, 128), F32)] * 4
    nk = 2
    z_spec = pl.BlockSpec((3, 2, nk, LZ, 128), lambda k: (0, 0, k, 0, 0))
    green = jnp.swapaxes(green_spectra, 2, 3).reshape(6, 2 * GZ, PX * PY)

    after = pl.BlockSpec(memory_space=pl.ANY)
    table_specs = [[pl.BlockSpec((GX, GX), lambda c, half=half: (0, half))] * 4 for half in range(2)]
    sent = []
    for half in range(2):
        earlier = [green, sent[0]] if half else []
        kernel = call(x_forward, (3,), [after] * len(earlier) + [latest_spec] + table_specs[half], row_spec, row_shape)
        sent.append(kernel(*earlier, krylov_basis, *x_tables))
    rows = [exchange_rows(x) for x in sent]
    back = [t.T for t in lax.optimization_barrier((*side, sent[0]))[:2]]
    own = [
        call(
            y_forward,
            (3,),
            [smem, row_spec, whole(side[0].shape), whole(side[1].shape)],
            [col_spec] * NCOL,
            [col_shape] * NCOL,
            turn,
        )(me, rows[half], *side)
        for half in range(2)
    ]
    cols = [exchange_cols(blocks) for blocks in own]
    mixed = []
    for half in range(2):
        mixed.append(
            call(
                z_both,
                (4 // nk,),
                [
                    after,
                    smem,
                    pl.BlockSpec((6, 2 * GZ, nk * 128), lambda k, half=half: (0, 0, half * (4 // nk) + k)),
                    whole(side[0].shape),
                    whole(side[1].shape),
                    whole(back[0].shape),
                    whole(back[1].shape),
                ]
                + [z_spec] * NCOL,
                [z_spec] * NCOL,
                [col_shape] * NCOL,
                [pltpu.VMEM((3, 2 * GZ, nk * 128), F32), pltpu.VMEM((3, 4 * GZ, nk * 128), F32)],
            )(own[1 - half][0], me, green, *side, *back, *cols[half])
        )
    cols = [exchange_cols(blocks) for blocks in mixed]
    sent = []
    for half in range(2):
        kernel = call(
            y_back,
            (3,),
            [after, smem, whole(back[0].shape), whole(back[1].shape)] + [col_spec] * NCOL,
            row_spec,
            row_shape,
            turn,
        )
        sent.append(kernel(mixed[1 - half][0], me, *back, *cols[half]))
    arrived = [exchange_rows(x) for x in sent]
    gram_part = call(basis_gram, (3,), [basis_spec], whole((1, 128)), line, (), HELD)(krylov_basis)
    chi_spec = whole((LZ, LY, GX))
    table_spec = pl.BlockSpec((4, GX, GX), lambda c: (0, 0, 0))
    first, table = call(
        x_back_first,
        (3,),
        [row_spec] + table_specs[0] + table_specs[1] + [latest_spec, chi_spec],
        [image_spec, table_spec],
        [jax.ShapeDtypeStruct((2, 3, ROOMY * LZ, LY, GX), F32), jax.ShapeDtypeStruct((6 * ROOMY, GX, GX), BF16)],
        (),
        HELD,
    )(arrived[0], *x_tables, *x_tables, krylov_basis, susceptibility)
    image, everyone = call(
        x_back,
        (3,),
        [row_spec, table_spec, image_spec, basis_spec, chi_spec, whole((1, 128))],
        [image_spec, whole((NROW * NCOL, 128))],
        [image_shape, jax.ShapeDtypeStruct((NROW * NCOL, 128), F32)],
        [pltpu.VMEM((1, 128), F32)],
        HELD,
    )(arrived[1], table, first, krylov_basis, susceptibility, gram_part)
    everyone = everyone.reshape(NROW * NCOL, 1, 128)
    everyone = lax.all_to_all(everyone, ROW_COL, split_axis=0, concat_axis=0, tiled=True)
    next_block, coefficients, factor = call(
        finish,
        (3,),
        [whole((NROW * NCOL, 128)), image_spec, basis_spec],
        [image_spec, smem, smem],
        [image_shape, jax.ShapeDtypeStruct((2, 2, NB), F32), jax.ShapeDtypeStruct((2, 2), F32)],
        [pltpu.VMEM((1, 128), F32), pltpu.SMEM((1, 128), F32), pltpu.VMEM((3, 8, 128), F32)],
        SMALL,
    )(everyone.reshape(NROW * NCOL, 128), image, krylov_basis)
    return (jnp.transpose(coefficients, (2, 0, 1)), next_block, factor)


def solution(mesh):
    split_mesh = Mesh(mesh.devices.reshape(4, 4, 4, 2), ("row_0", "row_1", "col_0", "col_1"))

    return jax.shard_map(
        per_device,
        mesh=split_mesh,
        in_specs=(P(None, None, None, COL, ROW, None), P(COL, ROW, None), P(None, None, COL, ROW)),
        out_specs=(P(), P(None, None, COL, ROW, None), P()),
        check_vma=False,
    )
```

```python
import functools
import math

import jax
import jax.numpy as jnp
import ml_dtypes
import numpy as np
from jax import lax
from jax.experimental import pallas as pl
from jax.experimental.pallas import tpu as pltpu
from jax.sharding import Mesh
from jax.sharding import PartitionSpec as P

GX = 256
GY = 128
GZ = 128
NB = 4
ROW = ("row_0", "row_1")
COL = ("col_0", "col_1")
ROW_COL = ROW + COL
NROW = 16
NCOL = 8
LZ = GZ // NCOL
LY = GY // NROW
PX = 2 * GX // NROW
HX = PX // 2
PY = 2 * GY // NCOL
F32 = jnp.float32
BF16 = jnp.bfloat16
ENTRY = 3.0 * GX * GY * GZ
SCALING = 1.0 / (8 * GX * GY * GZ)
PAIRS = [(i, k) for i in range(2 * NB) for k in range(i, 2 * NB)]
VMEM = 65024 * 1024
HELD = 40 * 1024 * 1024
ROOMY = 36
SMALL = 16 * 1024 * 1024


def split_np(table):
    table = table.astype(np.float32)
    high = table.astype(ml_dtypes.bfloat16)
    low = (table - high.astype(np.float32)).astype(ml_dtypes.bfloat16)
    return [high, low]


def tables():
    kx = np.arange(2 * GX).reshape(NROW, 2, PX // 2).transpose(1, 0, 2).reshape(-1)
    angle = (np.outer(np.arange(GX), kx) % (2 * GX)) * (2.0 * math.pi / (2 * GX))
    x_tables = split_np(np.cos(angle)) + split_np(np.sin(angle))
    angle = (np.outer(np.arange(2 * GY), np.arange(GY)) % (2 * GY)) * (2.0 * math.pi / (2 * GY))
    side = np.concatenate([np.cos(angle), np.sin(angle)], axis=0)
    return x_tables, split_np(side)


def split(x):
    high = x.astype(BF16)
    low = (x - high.astype(F32)).astype(BF16)
    return high, low


def dot(a, b, ca, cb):
    return lax.dot_general(a, b, (((ca,), (cb,)), ((), ())), preferred_element_type=F32)


def ahead(ref):
    c, s = ref[:256], ref[256:]
    return jnp.concatenate([jnp.concatenate([c, s], axis=1), jnp.concatenate([-s, c], axis=1)], axis=0)


def behind(ref):
    c, s = ref[:, :256], ref[:, 256:]
    return jnp.concatenate([jnp.concatenate([c, -s], axis=1), jnp.concatenate([s, c], axis=1)], axis=0)


def left(th, tl, x, cb):
    h, l = split(x)
    n = th.shape[0]
    wide = dot(jnp.concatenate([th, tl], axis=0), h, 1, cb)
    return wide[:n] + (wide[n:] + dot(th, l, 1, cb))


def right(x, th, tl, cb):
    h, l = split(x)
    n = x.shape[0]
    wide = dot(jnp.concatenate([h, l], axis=0), th, 1, cb)
    return wide[:n] + (wide[n:] + dot(h, tl, 1, cb))


def swap_blocks(v, width):
    v = list(v)
    block = lax.broadcasted_iota(jnp.int32, v[0].shape, 1) // width
    step = len(v) // 2
    while step:
        keep = (block & step) == 0
        for i in range(len(v)):
            if i & step == 0:
                p, q = v[i], v[i + step]
                v[i] = jnp.where(keep, p, pltpu.roll(q, step * width, 1))
                v[i + step] = jnp.where(keep, pltpu.roll(p, 128 - step * width, 1), q)
        step //= 2
    return v


def x_forward(half, *refs):
    u_hbm, *t_hbm = refs[-14:-9]
    o_hbm, u_ref, *t_ref = refs[-9:-3]
    o_ref, sem_in, sem_out = refs[-3:]
    n = LZ * LY
    tables = [
        pltpu.make_async_copy(t_hbm[i].at[:, pl.ds(half * GX, GX)], t_ref[i], sem_in.at[3 + i]) for i in range(4)
    ]
    fetch = lambda c: pltpu.make_async_copy(u_hbm.at[NB - 1, :, c], u_ref.at[c], sem_in.at[c])
    store = lambda c: pltpu.make_async_copy(o_ref.at[:, c], o_hbm.at[:, c], sem_out.at[c])
    fetch(0).start()
    for table in tables:
        table.start()
    fetch(1).start()
    fetch(2).start()
    for table in tables:
        table.wait()

    def body(c, carry):
        fetch(c).wait()
        u = u_ref[c].reshape(2 * n, GX)
        cos = right(u, t_ref[0][...], t_ref[1][...], 0)
        sin = right(u, t_ref[2][...], t_ref[3][...], 0)
        acc = jnp.concatenate([cos[:n] + sin[n:], cos[n:] - sin[:n]], axis=0)
        acc = acc.reshape(2, 2, 8, LY, GX)
        for t in range(2):
            part = acc[..., t * 128 : (t + 1) * 128]
            v = [part[:, :, zi].reshape(4 * LY, 128) for zi in range(8)]
            for di, w in enumerate(swap_blocks(v, HX)):
                o_ref[8 * t + di, c] = w.reshape(2, 2, LY, 128)
        store(c).start()
        return carry

    lax.fori_loop(0, 3, body, 0)
    for c in range(3):
        store(c).wait()


def y_forward(me_ref, x_ref, th_ref, tl_ref, *refs):
    o_refs, block_ref, s_refs = refs[:NCOL], refs[NCOL], refs[NCOL + 1 :]
    rows = []
    for zq in range(2):
        x = jnp.concatenate([x_ref[:, 0, r, zq].reshape(GY, 128) for r in range(2)], axis=0)
        rows.append(x.T)
    acc = right(jnp.concatenate(rows, axis=0), ahead(th_ref), ahead(tl_ref), 1)
    for r in range(2):
        for t in range(2):
            s_ref = s_refs[2 * r + t]
            lane = r * 256 + t * 128
            s_ref[...] = acc[:, lane : lane + 128]
            v = []
            for ki in range(4):
                v.append(jnp.concatenate([s_ref[pl.ds(4 * kq + ki, LZ, stride=HX), :] for kq in range(4)], axis=0))
            for ei, w in enumerate(swap_blocks(v, PY)):
                block_ref[4 * t + ei, r] = w.reshape(4, LZ, 128)
    for d in range(NCOL):
        o_refs[d][0] = block_ref[me_ref[0] ^ d]


def z_both(_, me_ref, g_ref, th_ref, tl_ref, bh_ref, bl_ref, *refs):
    x_refs, o_refs, s_ref, f_ref = refs[:NCOL], refs[NCOL : 2 * NCOL], refs[2 * NCOL], refs[2 * NCOL + 1]
    nk = x_refs[0].shape[2]

    def place(d, r):
        return pl.ds(pl.multiple_of(r * GZ + (me_ref[0] ^ d) * LZ, LZ), LZ)

    def there(c, carry):
        for d in range(NCOL):
            for r in range(2):
                for k in range(nk):
                    s_ref[c, place(d, r), k * 128 : (k + 1) * 128] = x_refs[d][c, r, k]
        f_ref[c] = left(ahead(th_ref), ahead(tl_ref), s_ref[c], 0)
        return carry

    def again(c, carry):
        pieces = []
        for r in range(2):
            total = None
            for j in range(3):
                entry = jnp.where(c == j, c, c + j + 2)
                term = g_ref[entry].astype(F32) * f_ref[j, r * 256 : (r + 1) * 256]
                total = term if total is None else total + term
            pieces.append(total)
        s_ref[c] = left(behind(bh_ref), behind(bl_ref), jnp.concatenate(pieces, axis=0), 0)
        for d in range(NCOL):
            for r in range(2):
                for k in range(nk):
                    o_refs[d][c, r, k] = s_ref[c, place(d, r), k * 128 : (k + 1) * 128]
        return carry

    lax.fori_loop(0, 3, there, 0)
    lax.fori_loop(0, 3, again, 0)


def y_back(_, me_ref, bh_ref, bl_ref, *refs):
    x_refs, o_ref, block_ref, s_refs = refs[:NCOL], refs[NCOL], refs[NCOL + 1], refs[NCOL + 2 :]
    for d in range(NCOL):
        block_ref[me_ref[0] ^ d] = x_refs[d][0]
    for r in range(2):
        for t in range(2):
            s_ref = s_refs[2 * r + t]
            v = [block_ref[4 * t + ei, r].reshape(4 * LZ, 128) for ei in range(4)]
            for ki, w in enumerate(swap_blocks(v, PY)):
                for kq in range(4):
                    s_ref[pl.ds(4 * kq + ki, LZ, stride=HX), :] = w[kq * LZ : (kq + 1) * LZ]
    x = jnp.concatenate([s_ref[...] for s_ref in s_refs], axis=1)
    acc = left(behind(bh_ref), behind(bl_ref), x, 1)
    for r in range(2):
        for zq in range(2):
            o_ref[:, 0, r, zq] = acc[r * GY : (r + 1) * GY, zq * 128 : (zq + 1) * 128].reshape(NROW, LY, 128)


def put_row(sums, first):
    rows = [jnp.sum(s, axis=0, keepdims=True) for s in sums]
    rows += [jnp.zeros((1, 128), F32)] * (-len(sums) % 8)
    stacked = jnp.concatenate(rows, axis=0)
    total = jnp.sum(stacked, axis=1, keepdims=True)
    row = lax.broadcasted_iota(jnp.int32, stacked.shape, 0)
    lane = lax.broadcasted_iota(jnp.int32, stacked.shape, 1)
    return jnp.sum(jnp.where(lane == row + first, total, 0.0), axis=0, keepdims=True)


def basis_gram(b_ref, o_ref):
    c = pl.program_id(0)
    zeros = tuple(jnp.zeros((8, 128), F32) for _ in PAIRS)

    def body(z, acc):
        for half in range(2):
            b = [b_ref[i // 2, i % 2, 0, z, :, half * 128 : (half + 1) * 128] for i in range(2 * NB)]
            acc = tuple(a + b[i] * b[k] for a, (i, k) in zip(acc, PAIRS))
        return acc

    acc = lax.fori_loop(0, LZ, body, zeros)

    @pl.when(c == 0)
    def _():
        o_ref[...] = jnp.zeros_like(o_ref)

    o_ref[...] += put_row(list(acc), 19)


def x_part(x_ref, ch_ref, cl_ref, sh_ref, sl_ref):
    n = LZ * LY
    planes = []
    for r in range(2):
        tiles = []
        for t in range(2):
            v = [x_ref[8 * t + di, 0, r].reshape(2 * LY, 128) for di in range(8)]
            w = [q.reshape(2, 1, LY, 128) for q in swap_blocks(v, HX)]
            tiles.append(jnp.concatenate(w, axis=1).reshape(n, 128))
        planes.append(jnp.concatenate(tiles, axis=1))
    planes = jnp.concatenate(planes, axis=0)
    cos = right(planes, ch_ref[...], cl_ref[...], 1)
    sin = right(planes, sh_ref[...], sl_ref[...], 1)
    return [(cos[:n] - sin[n:]).reshape(LZ, LY, GX), (cos[n:] + sin[:n]).reshape(LZ, LY, GX)]


def x_back_first(x_ref, ch_ref, cl_ref, sh_ref, sl_ref, *refs):
    others, (u_ref, chi_ref, o_ref, t_ref) = refs[:4], refs[4:]
    for place, other in enumerate(others):
        t_ref[place] = other[...]
    chi = chi_ref[...] * SCALING
    for j, part in enumerate(x_part(x_ref, ch_ref, cl_ref, sh_ref, sl_ref)):
        o_ref[j, 0] = u_ref[0, j, 0] - chi * part


def x_back(x_ref, t_ref, p_ref, b_ref, chi_ref, g_ref, img_ref, all_ref, o_ref):
    c = pl.program_id(0)
    chi = chi_ref[...] * SCALING
    for j, part in enumerate(x_part(x_ref, *(t_ref.at[place] for place in range(4)))):
        img_ref[j, 0] = p_ref[j, 0] - chi * part

    def body(z, sums):
        for half in range(2):
            lanes = slice(half * 128, (half + 1) * 128)
            b = [b_ref[i // 2, i % 2, 0, z, :, lanes] for i in range(2 * NB)]
            p = [img_ref[j, 0, z, :, lanes] for j in range(2)]
            terms = [b[i] * p[j] for i in range(2 * NB) for j in range(2)]
            terms += [p[0] * p[0], p[0] * p[1], p[1] * p[1]]
            sums = tuple(a + q for a, q in zip(sums, terms))
        return sums

    sums = lax.fori_loop(0, LZ, body, tuple(jnp.zeros((8, 128), F32) for _ in range(19)))

    @pl.when(c == 0)
    def _():
        o_ref[...] = g_ref[...]

    o_ref[...] += put_row(list(sums), 0)

    @pl.when(c == pl.num_programs(0) - 1)
    def _():
        all_ref[...] = jnp.broadcast_to(o_ref[...], all_ref.shape)


def finish(all_ref, img_ref, b_ref, o_ref, coef_ref, factor_ref, row_ref, s_ref, v_ref):
    @pl.when(pl.program_id(0) == 0)
    def _():
        row_ref[...] = jnp.sum(all_ref[...], axis=0, keepdims=True) / ENTRY
        pltpu.sync_copy(row_ref, s_ref)
        coef = [[s_ref[0, 2 * i + j] for j in range(2)] for i in range(2 * NB)]
        cells = [[None] * (2 * NB) for _ in range(2 * NB)]
        for place, (i, k) in enumerate(PAIRS):
            cells[i][k] = cells[k][i] = s_ref[0, 19 + place]
        mixed = []
        for i in range(2 * NB):
            entry = []
            for j in range(2):
                total = -2.0 * coef[i][j]
                for k in range(2 * NB):
                    total = total + cells[i][k] * coef[k][j]
                entry.append(total)
            mixed.append(entry)
        gram = []
        for place, (j, k) in enumerate(((0, 0), (0, 1), (1, 1))):
            total = s_ref[0, 16 + place]
            for i in range(2 * NB):
                total = total + coef[i][j] * mixed[i][k]
            gram.append(jnp.full((8, 128), total, F32))
        lead = jnp.sqrt(gram[0] + 1e-06)
        cross = gram[1] / lead
        tail = jnp.sqrt(gram[2] - cross * cross + 1e-06)
        v_ref[0] = 1.0 / lead
        v_ref[1] = cross
        v_ref[2] = 1.0 / tail
        for i in range(2 * NB):
            for j in range(2):
                coef_ref[i % 2, j, i // 2] = coef[i][j]
        factor_ref[0, 0] = lead[0, 0]
        factor_ref[0, 1] = cross[0, 0]
        factor_ref[1, 0] = 0.0
        factor_ref[1, 1] = tail[0, 0]

    def body(z, carry):
        for half in range(2):
            lanes = slice(half * 128, (half + 1) * 128)
            p0 = img_ref[0, 0, z, :, lanes]
            p1 = img_ref[1, 0, z, :, lanes]
            for i in range(2 * NB):
                b = b_ref[i // 2, i % 2, 0, z, :, lanes]
                p0 = p0 - s_ref[0, 2 * i] * b
                p1 = p1 - s_ref[0, 2 * i + 1] * b
            p0 = p0 * v_ref[0]
            o_ref[0, 0, z, :, lanes] = p0
            o_ref[1, 0, z, :, lanes] = (p1 - v_ref[1] * p0) * v_ref[2]
        return carry

    lax.fori_loop(0, LZ, body, 0)


def call(body, grid, ins, outs, shapes, scratch=(), grant=VMEM):
    return pl.pallas_call(
        body,
        grid=grid,
        in_specs=ins,
        out_specs=outs,
        out_shape=shapes,
        scratch_shapes=list(scratch),
        compiler_params=pltpu.CompilerParams(vmem_limit_bytes=grant, dimension_semantics=("arbitrary",) * len(grid) or None),
    )


def whole(shape):
    return pl.BlockSpec(shape, lambda *_: (0,) * len(shape))


def exchange_cols(blocks):
    moved = []
    for d in range(1, NCOL):
        moved.append(lax.ppermute(blocks[d], COL, [(i, i ^ d) for i in range(NCOL)]))
    return [blocks[0]] + moved


def exchange_rows(x):
    return lax.all_to_all(x, ROW, split_axis=0, concat_axis=0, tiled=True)


def per_device(krylov_basis, susceptibility, green_spectra):
    x_tables, side = ([jnp.asarray(t) for t in group] for group in tables())
    me = lax.axis_index(COL).astype(jnp.int32).reshape(1)
    row_spec = pl.BlockSpec((NROW, 1, 2, 2, LY, 128), lambda c: (0, c, 0, 0, 0, 0))
    row_shape = jax.ShapeDtypeStruct((NROW, 3, 2, 2, LY, 128), F32)
    col_spec = pl.BlockSpec((1, 2, 4, LZ, 128), lambda c: (c, 0, 0, 0, 0))
    col_shape = jax.ShapeDtypeStruct((3, 2, 4, LZ, 128), F32)
    latest_spec = pl.BlockSpec((1, 2, 1, LZ, LY, GX), lambda c: (NB - 1, 0, c, 0, 0, 0))
    basis_spec = pl.BlockSpec((NB, 2, 1, LZ, LY, GX), lambda c: (0, 0, c, 0, 0, 0))
    image_spec = pl.BlockSpec((2, 1, LZ, LY, GX), lambda c: (0, c, 0, 0, 0))
    image_shape = jax.ShapeDtypeStruct((2, 3, LZ, LY, GX), F32)
    line = jax.ShapeDtypeStruct((1, 128), F32)
    smem = pl.BlockSpec(memory_space=pltpu.SMEM)
    turn = [pltpu.VMEM((NCOL, 2, 4, LZ, 128), F32)] + [pltpu.VMEM((LZ * HX, 128), F32)] * 4
    nk = 2
    z_spec = pl.BlockSpec((3, 2, nk, LZ, 128), lambda k: (0, 0, k, 0, 0))
    green = jnp.swapaxes(green_spectra, 2, 3).reshape(6, 2 * GZ, PX * PY)

    after = pl.BlockSpec(memory_space=pl.ANY)
    table_specs = [[pl.BlockSpec((GX, GX), lambda c, half=half: (0, half))] * 4 for half in range(2)]
    sent = []
    for half in range(2):
        earlier = [green, sent[0]] if half else []
        kernel = call(
            functools.partial(x_forward, half),
            (),
            [after] * (len(earlier) + 5),
            after,
            row_shape,
            [pltpu.VMEM((3, 2, LZ, LY, GX), F32)]
            + [pltpu.VMEM((GX, GX), BF16)] * 4
            + [pltpu.VMEM((NROW, 3, 2, 2, LY, 128), F32)]
            + [pltpu.SemaphoreType.DMA((7,)), pltpu.SemaphoreType.DMA((3,))],
        )
        sent.append(kernel(*earlier, krylov_basis, *x_tables))
    rows = [exchange_rows(x) for x in sent]
    back = [t.T for t in lax.optimization_barrier((*side, sent[0]))[:2]]
    own = [
        call(
            y_forward,
            (3,),
            [smem, row_spec, whole(side[0].shape), whole(side[1].shape)],
            [col_spec] * NCOL,
            [col_shape] * NCOL,
            turn,
        )(me, rows[half], *side)
        for half in range(2)
    ]
    cols = [exchange_cols(blocks) for blocks in own]
    mixed = []
    for half in range(2):
        mixed.append(
            call(
                z_both,
                (4 // nk,),
                [
                    after,
                    smem,
                    pl.BlockSpec((6, 2 * GZ, nk * 128), lambda k, half=half: (0, 0, half * (4 // nk) + k)),
                    whole(side[0].shape),
                    whole(side[1].shape),
                    whole(back[0].shape),
                    whole(back[1].shape),
                ]
                + [z_spec] * NCOL,
                [z_spec] * NCOL,
                [col_shape] * NCOL,
                [pltpu.VMEM((3, 2 * GZ, nk * 128), F32), pltpu.VMEM((3, 4 * GZ, nk * 128), F32)],
            )(own[1 - half][0], me, green, *side, *back, *cols[half])
        )
    cols = [exchange_cols(blocks) for blocks in mixed]
    sent = []
    for half in range(2):
        kernel = call(
            y_back,
            (3,),
            [after, smem, whole(back[0].shape), whole(back[1].shape)] + [col_spec] * NCOL,
            row_spec,
            row_shape,
            turn,
        )
        sent.append(kernel(mixed[1 - half][0], me, *back, *cols[half]))
    arrived = [exchange_rows(x) for x in sent]
    gram_part = call(basis_gram, (3,), [basis_spec], whole((1, 128)), line, (), HELD)(krylov_basis)
    chi_spec = whole((LZ, LY, GX))
    table_spec = pl.BlockSpec((4, GX, GX), lambda c: (0, 0, 0))
    first, table = call(
        x_back_first,
        (3,),
        [row_spec] + table_specs[0] + table_specs[1] + [latest_spec, chi_spec],
        [image_spec, table_spec],
        [jax.ShapeDtypeStruct((2, 3, ROOMY * LZ, LY, GX), F32), jax.ShapeDtypeStruct((6 * ROOMY, GX, GX), BF16)],
        (),
        HELD,
    )(arrived[0], *x_tables, *x_tables, krylov_basis, susceptibility)
    image, everyone = call(
        x_back,
        (3,),
        [row_spec, table_spec, image_spec, basis_spec, chi_spec, whole((1, 128))],
        [image_spec, whole((NROW * NCOL, 128))],
        [image_shape, jax.ShapeDtypeStruct((NROW * NCOL, 128), F32)],
        [pltpu.VMEM((1, 128), F32)],
        HELD,
    )(arrived[1], table, first, krylov_basis, susceptibility, gram_part)
    everyone = everyone.reshape(NROW * NCOL, 1, 128)
    everyone = lax.all_to_all(everyone, ROW_COL, split_axis=0, concat_axis=0, tiled=True)
    next_block, coefficients, factor = call(
        finish,
        (3,),
        [whole((NROW * NCOL, 128)), image_spec, basis_spec],
        [image_spec, smem, smem],
        [image_shape, jax.ShapeDtypeStruct((2, 2, NB), F32), jax.ShapeDtypeStruct((2, 2), F32)],
        [pltpu.VMEM((1, 128), F32), pltpu.SMEM((1, 128), F32), pltpu.VMEM((3, 8, 128), F32)],
        SMALL,
    )(everyone.reshape(NROW * NCOL, 128), image, krylov_basis)
    return (jnp.transpose(coefficients, (2, 0, 1)), next_block, factor)


def solution(mesh):
    split_mesh = Mesh(mesh.devices.reshape(4, 4, 4, 2), ("row_0", "row_1", "col_0", "col_1"))

    return jax.shard_map(
        per_device,
        mesh=split_mesh,
        in_specs=(P(None, None, None, COL, ROW, None), P(COL, ROW, None), P(None, None, COL, ROW)),
        out_specs=(P(), P(None, None, COL, ROW, None), P()),
        check_vma=False,
    )
```
